1024 devices in a mesh: ctx: 64 (over z, y_lo, core), head: 16 (over y_hi, x).
Axes of the slice: x: 4, y: 8 (y_hi: 4, y_lo: 2; y = y_hi * 2 + y_lo), z: 16, core: 2. Of those that a mesh axis runs over, the one named last changes fastest.
Arguments:
- q_latent: bfloat16 [8192, 128, 512], P('ctx', 'head'), may hold values from -4 to 4
- q_rope: bfloat16 [8192, 8192], P('ctx', 'head'), may hold values from -5 to 5
- latent: bfloat16 [8192, 512], P('ctx'), may hold values from -5 to 5
- key_rope: bfloat16 [8192, 64], P('ctx'), may hold values from -5 to 5
- out_grad: bfloat16 [8192, 128, 512], P('ctx', 'head'), may hold values from -5 to 5
- inputs: bfloat16 [8192, 7168], P('ctx', 'head'), may hold values from -5 to 5
- doc_ids: int32 [8192], replicated, may hold values from 0 to 7, never falling along the last dimension, each value on 1 to 2048 neighbouring positions
Outputs:
- q_latent_grad: bfloat16 [8192, 128, 512], P('ctx', 'head')
- q_rope_grad: bfloat16 [8192, 8192], P('ctx', 'head')
- latent_grad: bfloat16 [8192, 512], P('ctx')
- key_rope_grad: bfloat16 [8192, 64], P('ctx')
- proj_grad: float32 [512, 7168], P('ctx', 'head')
The draws below stay inside these ranges and needn't reach their ends.
Inputs may be any that keep to these rules, and one draw needn't show every extreme that they name: `doc_ids`: ids never fall along the sequence; each document has at most 2048 positions.
All inputs are finite; a program needn't handle non-finite values.
Results may differ from the reference program's by a relative error of at most 0.0058.
Values may be sent and summed in bfloat16 or wider, within the bound.
A program may use at most 32 MiB of HBM per device.

```python
import math
import jax
import jax.numpy as jnp
import numpy as np
from jax import lax

D = 7168
HEADS = 128
KVL = 512
ROPE = 64
TOK_DEV = 128
WINDOW = 384
KEYS = 512
TOKENS = 8192
N_CTX = 64


def draw_latent(key, part):
    values = jnp.clip(jax.random.normal(jax.random.fold_in(key, 11), (TOKENS, KVL), jnp.float32), -5.0, 5.0)
    return values.astype(jnp.bfloat16)


def draw_q_latent(key, part):
    values = jnp.clip(0.5 * jax.random.normal(jax.random.fold_in(key, 13), (TOKENS, HEADS, KVL), jnp.float32), -4.0, 4.0)
    return values.astype(jnp.bfloat16)


def shard_levels(key, shape, shards, smallest, largest):
    factor_of, own = 1.0, jax.random.fold_in(key, 6)
    for position, shards_of in shards:
        heights = jnp.exp(jax.random.uniform(jax.random.fold_in(own, position), (shards_of,), jnp.float32, smallest / len(shards), largest / len(shards)))
        factor_of = factor_of * jnp.repeat(heights, shape[position] // shards_of).reshape([-1 if axis == position else 1 for axis in range(len(shape))])
    return factor_of


def profile(count, total, most, lean):
    loads = [(1 << 20) // math.isqrt(rank ** lean) + 1 for rank in range(2, count + 1)]
    rest, counts = total - most - (count - 1), [1] * (count - 1)
    while rest > 0:
        candidates = [i for i in range(count - 1) if counts[i] < most]
        mass, remaining = sum([loads[i] for i in candidates]), rest
        for i in candidates:
            addition = min(most - counts[i], max(1, remaining * loads[i] // mass), rest)
            counts[i] = counts[i] + addition
            rest = rest - addition
    return np.array([most] + counts)


def ragged_sizes(stream_key, number_of, total, most, slope):
    if number_of == 2:
        one = jax.random.randint(stream_key, (), max(1, total - most), min(most, total - 1) + 1)
        return jnp.stack([one, total - one])
    tallies = jnp.asarray(profile(number_of, total, most, slope), jnp.int32)
    twos = (number_of - 1) // 2
    giver, taker = tallies[1:1 + 2 * twos:2], tallies[2:2 + 2 * twos:2]
    slack = jnp.minimum(giver - 1, most - taker)
    passed = jax.random.randint(jax.random.fold_in(stream_key, 1), (twos,), 0, 1 << 20) % (slack + 1)
    tallies = tallies.at[1:1 + 2 * twos:2].set(giver - passed).at[2:2 + 2 * twos:2].set(taker + passed)
    return tallies[jax.random.permutation(jax.random.fold_in(stream_key, 2), number_of)]


def gaussian(own_key, extent, scale, bound, split=(), kind=jnp.bfloat16):
    array = scale * jax.random.normal(own_key, extent, jnp.float32)
    if split:
        array = array * shard_levels(own_key, extent, split, -0.22, 0.18)
    return jnp.clip(array, -bound, bound).astype(kind)


def setup_inputs(seed: int = 0) -> dict:
    keys = jax.random.split(jax.random.key(seed), 8)
    return {
        "q_latent": draw_q_latent(jax.random.fold_in(keys[7], 71), 0),
        "q_rope": gaussian(keys[1], (TOKENS, HEADS * ROPE), 1.0, 5.0, ((0, 64), (1, 16))),
        "latent": draw_latent(jax.random.fold_in(keys[7], 71), 0),
        "key_rope": gaussian(keys[3], (TOKENS, ROPE), 1.0, 5.0, ((0, 64),)),
        "out_grad": gaussian(keys[4], (TOKENS, HEADS, KVL), 1.0, 5.0, ((0, 64), (1, 16))),
        "inputs": gaussian(keys[5], (TOKENS, D), 1.0, 5.0, ((0, 64), (1, 16))),
        "doc_ids": jnp.searchsorted(jnp.cumsum(ragged_sizes(keys[6], 8, TOKENS, TOKENS // 4, 1)), jnp.arange(TOKENS), side="right").astype(jnp.int32),
    }


softmax_scale = 192.0 ** -0.5


def reference(q_latent, q_rope, latent, key_rope, out_grad, inputs, doc_ids):
    lat_pad = jnp.concatenate([jnp.zeros((WINDOW, KVL), jnp.float32), latent.astype(jnp.float32)], axis=0)
    rope_pad = jnp.concatenate([jnp.zeros((WINDOW, ROPE), jnp.float32), key_rope.astype(jnp.float32)], axis=0)
    doc_pad = jnp.concatenate([jnp.full((WINDOW,), -1, jnp.int32), doc_ids.astype(jnp.int32)], axis=0)
    qrope_all = q_rope.reshape(TOKENS, HEADS, ROPE)

    def block_step(carry, block):
        acc_lat, acc_rope = carry
        start = (block * TOK_DEV).astype(jnp.int32)
        qlat = lax.dynamic_slice_in_dim(q_latent, start, TOK_DEV, 0).astype(jnp.float32)
        qrot = lax.dynamic_slice_in_dim(qrope_all, start, TOK_DEV, 0).astype(jnp.float32)
        grad_out = lax.dynamic_slice_in_dim(out_grad, start, TOK_DEV, 0).astype(jnp.float32)
        keys_lat = lax.dynamic_slice_in_dim(lat_pad, start, KEYS, 0)
        keys_rope = lax.dynamic_slice_in_dim(rope_pad, start, KEYS, 0)
        key_doc = lax.dynamic_slice_in_dim(doc_pad, start, KEYS, 0)
        query_doc = lax.dynamic_slice_in_dim(doc_ids.astype(jnp.int32), start, TOK_DEV, 0)
        qpos = jnp.arange(TOK_DEV, dtype=jnp.int32)
        kpos = jnp.arange(KEYS, dtype=jnp.int32) - WINDOW
        allowed = (kpos[None, :] <= qpos[:, None]) & (qpos[:, None] - kpos[None, :] < WINDOW) & (key_doc[None, :] == query_doc[:, None])
        scores = (jnp.einsum("thj,kj->thk", qlat, keys_lat) + jnp.einsum("thr,kr->thk", qrot, keys_rope)) * softmax_scale
        masked = jnp.where(allowed[:, None, :], scores, -jnp.inf)
        top = jnp.max(masked, axis=-1, keepdims=True)
        expo = jnp.exp(masked - top)
        probs = expo / jnp.sum(expo, axis=-1, keepdims=True)
        probs_low = lax.optimization_barrier(probs.astype(jnp.bfloat16)).astype(jnp.float32)
        merged = jnp.einsum("thk,kj->thj", probs_low, keys_lat)
        delta = jnp.sum(grad_out * merged, axis=-1)
        dprob = jnp.einsum("thj,kj->thk", grad_out, keys_lat)
        dscore = (probs * (dprob - delta[..., None]) * softmax_scale)
        dscore = lax.optimization_barrier(dscore.astype(jnp.bfloat16)).astype(jnp.float32)
        grad_qlat = jnp.einsum("thk,kj->thj", dscore, keys_lat).astype(jnp.bfloat16)
        grad_qrope = jnp.einsum("thk,kr->thr", dscore, keys_rope).reshape(TOK_DEV, HEADS * ROPE).astype(jnp.bfloat16)
        part_lat = jnp.einsum("thk,thj->kj", dscore, qlat) + jnp.einsum("thk,thj->kj", probs_low, grad_out)
        part_rope = jnp.einsum("thk,thr->kr", dscore, qrot)
        acc_lat = lax.dynamic_update_slice_in_dim(acc_lat, lax.dynamic_slice_in_dim(acc_lat, start, KEYS, 0) + part_lat, start, 0)
        acc_rope = lax.dynamic_update_slice_in_dim(acc_rope, lax.dynamic_slice_in_dim(acc_rope, start, KEYS, 0) + part_rope, start, 0)
        return (acc_lat, acc_rope), (grad_qlat, grad_qrope)

    init = (jnp.zeros((WINDOW + TOKENS, KVL), jnp.float32), jnp.zeros((WINDOW + TOKENS, ROPE), jnp.float32))
    (acc_lat, acc_rope), (grads_qlat, grads_qrope) = lax.scan(block_step, init, jnp.arange(N_CTX, dtype=jnp.int32))
    q_latent_grad = grads_qlat.reshape(TOKENS, HEADS, KVL)
    q_rope_grad = grads_qrope.reshape(TOKENS, HEADS * ROPE)
    latent_grad = acc_lat[WINDOW:].astype(jnp.bfloat16)
    key_rope_grad = acc_rope[WINDOW:].astype(jnp.bfloat16)
    proj_grad = jnp.dot(latent_grad.T, inputs, preferred_element_type=jnp.float32)
    return q_latent_grad, q_rope_grad, latent_grad, key_rope_grad, proj_grad
```

```python
import functools

import jax
import jax.numpy as jnp
from jax import lax
from jax.experimental import pallas as pl
from jax.experimental.pallas import tpu as pltpu
from jax.sharding import PartitionSpec as P

MESH = pl.DeviceIdType.MESH
BF16, F32 = jnp.bfloat16, jnp.float32
SCALE = 192.0 ** (-0.5)
FAR = -1e30
EXT = 128
QUAD = 4
SLOTS = 4
NT = (((1,), (1,)), ((), ()))
TN = (((0,), (0,)), ((), ()))


def dot(a, b, dims=(((1,), (0,)), ((), ()))):
    return lax.dot_general(a, b, dims, preferred_element_type=F32)


def iota(shape, dim):
    return lax.broadcasted_iota(jnp.int32, shape, dim)


def kernel(cfg, q_hbm, qr_hbm, lat_hbm, rope_hbm, og_hbm, in_hbm, doc_hbm,
           dq_hbm, dqr_hbm, lg_hbm, krg_hbm, pg_hbm,
           qx, og, qr, keys, rope, inp, doc, perm, st, dt, probs, dscore, part, xbuf, ysend, ybuf,
           gbuf, latp, ebuf, zsend, zbuf, dq, dqr, krx, pg, hot, pick, drop,
           load_sem, hs_sem, hr_sem, xs_sem, xr_sem, ys_sem, yr_sem, gs_sem, gr_sem,
           es_sem, er_sem, is_sem, ir_sem, zs_sem, zr_sem, out_sem):
    n_ctx, n_z, n_yh, n_x, tok, wid, heads = cfg
    rows = tok * heads
    n_head = n_yh * n_x
    full = wid + EXT
    c, h = lax.axis_index("ctx"), lax.axis_index("head")
    z, quad = lax.div(c, QUAD), lax.rem(c, QUAD)
    yh, x = lax.div(h, n_x), lax.rem(h, n_x)
    own = (SLOTS - 1) * tok
    chunks = [(0, wid // 2), (wid // 2, wid // 2), (wid, EXT)]

    def ctx_at(by):
        return lax.rem(c + (by + n_ctx), n_ctx)

    def yh_at(by):
        return lax.rem(yh + by, n_yh)

    def x_at(by):
        return lax.rem(x + by, n_x)

    def quad_at(by):
        return z * QUAD + lax.rem(quad + by, QUAD)

    def z_at(by):
        return lax.rem(z + by, n_z) * QUAD + quad

    def near(ref_a, ref_b, sem):
        return pltpu.make_async_copy(ref_a, ref_b, sem)

    def send(src, dst, ssem, rsem, ci, hi):
        copy = pltpu.make_async_remote_copy(
            src_ref=src, dst_ref=dst, send_sem=ssem, recv_sem=rsem, device_id=(ci, hi), device_id_type=MESH
        )
        copy.start()
        return copy

    barrier = pltpu.get_barrier_semaphore()
    count = 0
    for by in range(-3, 4):
        for e in range(n_yh):
            if by or e:
                pl.semaphore_signal(barrier, inc=1, device_id=(ctx_at(by), yh_at(e) * n_x + x), device_id_type=MESH)
                count += 1
    for d in range(1, n_x):
        for e in range(n_yh):
            pl.semaphore_signal(barrier, inc=1, device_id=(c, yh_at(e) * n_x + x_at(d)), device_id_type=MESH)
            count += 1
    for d in range(1, n_z):
        pl.semaphore_signal(barrier, inc=1, device_id=(z_at(d), h), device_id_type=MESH)
        count += 1

    loads = [
        near(doc_hbm.at[c], doc, load_sem.at[0]),
        near(rope_hbm, rope, load_sem.at[1]),
        near(lat_hbm, keys.at[pl.ds(own, tok), pl.ds(0, wid)], load_sem.at[2]),
        near(qr_hbm, qr, load_sem.at[3]),
        near(q_hbm, qx.at[:, pl.ds(0, wid)], load_sem.at[4]),
        near(og_hbm, og, load_sem.at[5]),
        near(in_hbm, inp.at[0], load_sem.at[6]),
    ]
    for copy in loads:
        copy.start()

    n_rope = rope.shape[0]
    loads[0].wait()
    loads[1].wait()
    ids = doc[...]
    lane_t = iota((EXT, tok), 0)
    here_t = (lane_t - n_rope == ids).astype(F32).astype(BF16)
    tag_rows = (lane_t >= n_rope) & (lane_t < n_rope + 8)
    away_t = jnp.where(tag_rows & (lane_t - n_rope != ids), FAR, 0.0).astype(BF16)
    eye = (iota((tok, tok), 0) == iota((tok, tok), 1)).astype(F32).astype(BF16)
    here = dot(eye, here_t, NT).astype(BF16)
    tagged = jnp.concatenate([rope[...].astype(F32), away_t[n_rope:].astype(F32)], axis=0).astype(BF16)
    keys[pl.ds(own, tok), pl.ds(wid, EXT)] = dot(eye, tagged, NT).astype(BF16)
    loads[2].wait()

    pl.semaphore_wait(barrier, count)
    halo = [
        send(keys.at[pl.ds(own, tok)], keys.at[pl.ds((3 - by) * tok, tok)], hs_sem.at[by - 1], hr_sem.at[by - 1],
             ctx_at(by), h)
        for by in (3, 2, 1)
    ]

    step = min(rows, 128)
    per = step // heads
    cols = heads * n_rope
    spread = (lax.div(iota((step, per), 0), heads) == iota((step, per), 1)).astype(F32).astype(BF16)
    gather = (lax.div(iota((per, step), 1), heads) == iota((per, step), 0)).astype(F32).astype(BF16)
    head_of = (lax.div(iota((step, cols), 1), n_rope) == lax.rem(iota((step, cols), 0), heads)).astype(F32)
    hot[...] = here
    pick[...] = (lax.rem(iota((cols, EXT), 0), n_rope) == iota((cols, EXT), 1)).astype(F32).astype(BF16)
    drop[...] = (lax.rem(iota((EXT, cols), 1), n_rope) == iota((EXT, cols), 0)).astype(F32).astype(BF16)
    line, place_of = iota((wid, wid), 0), iota((wid, wid), 1)
    target = lax.rem(lax.div(line, 8), n_z) * (8 * QUAD) + lax.div(line, 8 * n_z) * 8 + lax.rem(line, 8)
    perm[...] = (target == place_of).astype(F32).astype(BF16)
    loads[3].wait()

    @pl.loop(0, rows // step)
    def _(i):
        ts = pl.ds(pl.multiple_of(i * per, per), per)
        rs = pl.ds(pl.multiple_of(i * step, step), step)
        wide = (dot(spread, qr[ts, :]) * head_of).astype(BF16)
        qx[rs, pl.ds(wid, EXT)] = (dot(wide, pick[...]) + dot(spread, hot[ts, :])).astype(BF16)

    loads[4].wait()
    loads[5].wait()
    big = min(rows, 256)

    def score(k0, k1):
        @pl.loop(0, rows // big)
        def _(i):
            rs = pl.ds(pl.multiple_of(i * big, big), big)
            st[pl.ds(k0, k1 - k0), rs] = dot(keys[pl.ds(k0, k1 - k0), :], qx[rs, :], NT)
            dt[pl.ds(k0, k1 - k0), rs] = dot(keys[pl.ds(k0, k1 - k0), pl.ds(0, wid)], og[rs, :], NT)

    score(own, own + tok)
    for copy in halo:
        copy.wait_recv()
    loads[6].wait()
    swap = [send(inp.at[0], inp.at[d], is_sem.at[d - 1], ir_sem.at[d - 1], quad_at(d), h) for d in (1, 2, 3)]
    score(0, own)

    @pl.loop(0, rows // step)
    def _(i):
        rs = pl.ds(pl.multiple_of(i * step, step), step)
        row = iota((tok, step), 0)
        t = i * per + lax.div(iota((tok, step), 1), heads)
        first = jnp.where(row > t, st[pl.ds(0, tok), rs], FAR)
        last = jnp.where(row <= t, st[pl.ds(own, tok), rs], FAR)
        s = jnp.concatenate([first, st[pl.ds(tok, own - tok), rs], last], axis=0) * SCALE
        e = jnp.exp(s - jnp.max(s, axis=0, keepdims=True))
        p = e * (1.0 / jnp.sum(e, axis=0, keepdims=True))
        low = p.astype(BF16)
        dp = dt[:, rs]
        delta = jnp.sum(low.astype(F32) * dp, axis=0, keepdims=True)
        probs[:, rs] = low
        dscore[:, rs] = (p * (dp - delta) * SCALE).astype(BF16)

    x_sends = []
    for k, (c0, cc) in enumerate(chunks):
        at = pl.ds(c0, cc)
        total = dot(dscore[...], qx[:, at])
        if c0 < wid:
            total = total + dot(probs[...], og[:, at])
        total = total.astype(BF16).reshape(SLOTS, n_x, tok // n_x, cc)
        for xi in range(n_x):
            part[xi, :, :, at] = total[:, xi]
        x_sends.append([
            send(part.at[x_at(d), :, :, at], xbuf.at[d - 1, :, :, at], xs_sem.at[d - 1, k], xr_sem.at[d - 1, k],
                 c, yh * n_x + x_at(d))
            for d in range(1, n_x)
        ])

    @pl.loop(0, rows // step)
    def _(i):
        ts = pl.ds(pl.multiple_of(i * per, per), per)
        rs = pl.ds(pl.multiple_of(i * step, step), step)
        g = dot(dscore[:, rs], keys[...], TN)
        dq[rs, :] = g[:, :wid].astype(BF16)
        wide = (dot(g[:, wid:].astype(BF16), drop[...]) * head_of).astype(BF16)
        dqr[ts, :] = dot(gather, wide).astype(BF16)

    outs = [near(dq, dq_hbm, out_sem.at[0]), near(dqr, dqr_hbm, out_sem.at[1])]
    for copy in outs:
        copy.start()

    y_sends = []
    for k, (c0, cc) in enumerate(chunks):
        at = pl.ds(c0, cc)
        for copy in x_sends[k]:
            copy.wait_recv()
        total = part[x, :, :, at].astype(F32)
        for d in range(1, n_x):
            total = total + xbuf[d - 1, :, :, at].astype(F32)
        total = total.reshape(SLOTS, n_yh, 8, cc).astype(BF16)
        for yi in range(n_yh):
            ysend[yi, :, :, at] = total[:, yi]
        for s in range(SLOTS):
            for e in range(n_yh):
                if s < SLOTS - 1 or e:
                    y_sends.append(
                        send(ysend.at[yh_at(e), s, :, at], ybuf.at[s * n_yh + e, :, at], ys_sem.at[k, s * n_yh + e],
                             yr_sem.at[k, s * n_yh + e], ctx_at(s - 3), yh_at(e) * n_x + x))

    def all_of(k, group):
        size = (SLOTS * n_yh - 1)
        return group[k * size:(k + 1) * size]

    place_here = x * n_yh + yh
    g_sends = []
    for k, (c0, cc) in enumerate(chunks):
        at = pl.ds(c0, cc)
        for copy in all_of(k, y_sends):
            copy.wait_recv()
        total = ysend[yh, SLOTS - 1, :, at].astype(F32)
        for m in range(SLOTS * n_yh):
            if m != (SLOTS - 1) * n_yh:
                total = total + ybuf[m, :, at].astype(F32)
        gbuf[place_here, :, at] = total.astype(BF16)
        for d in range(n_x):
            for e in range(n_yh):
                if d or e:
                    g_sends.append(
                        send(gbuf.at[place_here, :, at], gbuf.at[place_here, :, at], gs_sem.at[k, d * n_yh + e],
                             gr_sem.at[k, d * n_yh + e], c, yh_at(e) * n_x + x_at(d)))

    def gathered(k):
        size = n_head - 1
        for copy in g_sends[k * size:(k + 1) * size]:
            copy.wait_recv()

    gathered(0)
    gathered(1)
    outs.append(near(gbuf.at[:, :, pl.ds(0, wid)], lg_hbm, out_sem.at[2]))
    outs[-1].start()
    whole = gbuf[:, :, pl.ds(0, wid)].astype(F32).reshape(tok, wid).astype(BF16)
    latp[...] = dot(perm[...], whole, NT).astype(BF16).reshape(QUAD, 8 * n_z, tok)
    e_sends = [
        send(latp.at[lax.rem(quad + d, QUAD)], ebuf.at[d - 1], es_sem.at[d - 1], er_sem.at[d - 1], quad_at(d), h)
        for d in (1, 2, 3)
    ]
    total = dot(latp[quad], inp[0], NT)
    for d in (1, 2, 3):
        swap[d - 1].wait_recv()
        e_sends[d - 1].wait_recv()
        total = total + dot(ebuf[d - 1], inp[d], NT)
    zsend[...] = total.reshape(n_z, 8, total.shape[1]).astype(BF16)
    z_sends = [
        send(zsend.at[lax.rem(z + d, n_z)], zbuf.at[d - 1], zs_sem.at[d - 1], zr_sem.at[d - 1], z_at(d), h)
        for d in sorted(range(1, n_z), key=lambda d: -min(d, n_z - d))
    ]
    gathered(2)
    ext = gbuf[:, :, pl.ds(wid, EXT)].astype(F32).reshape(tok, EXT).astype(BF16)
    take = (iota((n_rope, EXT), 0) == iota((n_rope, EXT), 1)).astype(F32).astype(BF16)
    krx[...] = dot(take, ext, NT).astype(BF16)
    outs.append(near(krx, krg_hbm, out_sem.at[3]))
    outs[-1].start()
    total = zsend[z].astype(F32)
    for copy in z_sends:
        copy.wait_recv()
    for d in range(1, n_z):
        total = total + zbuf[d - 1].astype(F32)
    pg[...] = total
    outs.append(near(pg, pg_hbm, out_sem.at[4]))
    outs[-1].start()
    for copy in halo + swap + sum(x_sends, []) + y_sends + g_sends + e_sends + z_sends:
        copy.wait_send()
    for copy in outs:
        copy.wait()


def solution(mesh):
    n_ctx, n_head = mesh.shape["ctx"], mesh.shape["head"]
    n_x = 4 if n_head == 16 else 2
    n_yh = n_head // n_x
    n_z = n_ctx // QUAD

    def shards(q_latent, q_rope, latent, key_rope, out_grad, inputs, doc_ids):
        tok, heads, wid = q_latent.shape
        n_rope, dloc = key_rope.shape[1], inputs.shape[1]
        rows, full, keys = tok * heads, wid + EXT, SLOTS * tok
        cfg = (n_ctx, n_z, n_yh, n_x, tok, wid, heads)
        vm = pltpu.VMEM
        dma = pltpu.SemaphoreType.DMA
        y_n = SLOTS * n_yh
        shape = jax.ShapeDtypeStruct
        anywhere = pl.BlockSpec(memory_space=pl.ANY)
        outs = pl.pallas_call(
            functools.partial(kernel, cfg),
            out_shape=(
                shape((rows, wid), BF16),
                shape((tok, heads * n_rope), BF16),
                shape((n_head, 8, wid), BF16),
                shape((n_rope, tok), BF16),
                shape((8, dloc), F32),
            ),
            in_specs=[anywhere] * 7,
            out_specs=(anywhere,) * 5,
            scratch_shapes=[
                vm((rows, full), BF16), vm((rows, wid), BF16), vm((tok, heads * n_rope), BF16),
                vm((keys, full), BF16), vm((n_rope, tok), BF16), vm((QUAD, dloc, tok), BF16),
                vm((1, tok), jnp.int32), vm((wid, wid), BF16),
                vm((keys, rows), F32), vm((keys, rows), F32), vm((keys, rows), BF16), vm((keys, rows), BF16),
                vm((n_x, SLOTS, tok // n_x, full), BF16), vm((n_x - 1, SLOTS, tok // n_x, full), BF16),
                vm((n_yh, SLOTS, 8, full), BF16), vm((y_n, 8, full), BF16),
                vm((n_head, 8, full), BF16), vm((QUAD, 8 * n_z, tok), BF16), vm((QUAD - 1, 8 * n_z, tok), BF16),
                vm((n_z, 8, dloc), BF16), vm((n_z - 1, 8, dloc), BF16),
                vm((rows, wid), BF16), vm((tok, heads * n_rope), BF16), vm((n_rope, tok), BF16),
                vm((8, dloc), F32), vm((tok, EXT), BF16), vm((heads * n_rope, EXT), BF16), vm((EXT, heads * n_rope), BF16),
                dma((7,)), dma((3,)), dma((3,)), dma((n_x - 1, 3)), dma((n_x - 1, 3)), dma((3, y_n)), dma((3, y_n)),
                dma((3, n_head)), dma((3, n_head)), dma((3,)), dma((3,)), dma((3,)), dma((3,)),
                dma((n_z - 1,)), dma((n_z - 1,)), dma((5,)),
            ],
            compiler_params=pltpu.CompilerParams(collective_id=0, has_side_effects=True),
            name="step",
        )(
            q_latent.reshape(rows, wid), q_rope, latent, key_rope.T, out_grad.reshape(rows, wid), inputs.T,
            doc_ids.reshape(n_ctx, 1, tok),
        )
        return (outs[0].reshape(tok, heads, wid), outs[1], outs[2].reshape(tok, wid), outs[3].T, outs[4])

    return jax.shard_map(
        shards,
        mesh=mesh,
        in_specs=(P("ctx", "head", None), P("ctx", "head"), P("ctx", None), P("ctx", None), P("ctx", "head", None),
                  P("ctx", "head"), P()),
        out_specs=(P("ctx", "head", None), P("ctx", "head"), P("ctx", None), P("ctx", None), P("ctx", "head")),
        check_vma=False,
    )
```

```python
import functools

import jax
import jax.numpy as jnp
from jax import lax
from jax.experimental import pallas as pl
from jax.experimental.pallas import tpu as pltpu
from jax.sharding import PartitionSpec as P

MESH = pl.DeviceIdType.MESH
BF16, F32 = jnp.bfloat16, jnp.float32
SCALE = 192.0 ** (-0.5)
FAR = -1e30
EXT = 128
QUAD = 4
SLOTS = 4
NT = (((1,), (1,)), ((), ()))
TN = (((0,), (0,)), ((), ()))


def dot(a, b, dims=(((1,), (0,)), ((), ()))):
    return lax.dot_general(a, b, dims, preferred_element_type=F32)


def iota(shape, dim):
    return lax.broadcasted_iota(jnp.int32, shape, dim)


def kernel(cfg, q_hbm, qr_hbm, lat_hbm, rope_hbm, og_hbm, in_hbm, doc_hbm,
           dq, dqr, lg_out, krx, pg_out,
           qx, og, qr, keys, rope, inp, doc, perm, st, dt, weights, both, part, xbuf, ysend, ybuf,
           gbuf, tbuf, zsend, zbuf, hot, pick, drop,
           load_sem, hs_sem, hr_sem, xs_sem, xr_sem, ys_sem, yr_sem, gs_sem, gr_sem,
           ts_sem, tr_sem, is_sem, ir_sem, zs_sem, zr_sem):
    n_ctx, n_z, n_yh, n_x, tok, wid, heads = cfg
    rows = tok * heads
    n_head = n_yh * n_x
    full = wid + EXT
    c, h = lax.axis_index("ctx"), lax.axis_index("head")
    z, quad = lax.div(c, QUAD), lax.rem(c, QUAD)
    yh, x = lax.div(h, n_x), lax.rem(h, n_x)
    own = (SLOTS - 1) * tok
    y_n = SLOTS * n_yh
    chunks = [(0, wid // 2), (wid // 2, wid // 2), (wid, EXT)]

    def ctx_at(by):
        return lax.rem(c + (by + n_ctx), n_ctx)

    def yh_at(by):
        return lax.rem(yh + by, n_yh)

    def x_at(by):
        return lax.rem(x + by, n_x)

    def quad_at(by):
        return z * QUAD + lax.rem(quad + by, QUAD)

    def z_at(by):
        return lax.rem(z + by, n_z) * QUAD + quad

    def near(ref_a, ref_b, sem):
        return pltpu.make_async_copy(ref_a, ref_b, sem)

    def send(src, dst, ssem, rsem, ci, hi):
        copy = pltpu.make_async_remote_copy(
            src_ref=src, dst_ref=dst, send_sem=ssem, recv_sem=rsem, device_id=(ci, hi), device_id_type=MESH
        )
        copy.start()
        return copy

    def group(ref, ssem, rsem):
        return pltpu.make_async_remote_copy(
            src_ref=ref, dst_ref=ref, send_sem=ssem, recv_sem=rsem, device_id=(c, h), device_id_type=MESH
        )

    barrier = pltpu.get_barrier_semaphore()
    count = 0
    for by in range(-3, 4):
        for e in range(n_yh):
            if by or e:
                pl.semaphore_signal(barrier, inc=1, device_id=(ctx_at(by), yh_at(e) * n_x + x), device_id_type=MESH)
                count += 1
    for d in range(1, n_x):
        for e in range(n_yh):
            pl.semaphore_signal(barrier, inc=1, device_id=(c, yh_at(e) * n_x + x_at(d)), device_id_type=MESH)
            count += 1
    for by in range(1, QUAD):
        for d in range(1, n_x):
            for e in range(n_yh):
                pl.semaphore_signal(
                    barrier, inc=1, device_id=(quad_at(by), yh_at(e) * n_x + x_at(d)), device_id_type=MESH)
                count += 1
    for d in range(1, n_z):
        pl.semaphore_signal(barrier, inc=1, device_id=(z_at(d), h), device_id_type=MESH)
        count += 1

    loads = [
        near(doc_hbm.at[c], doc, load_sem.at[0]),
        near(rope_hbm, rope, load_sem.at[1]),
        near(lat_hbm, keys.at[pl.ds(own, tok), pl.ds(0, wid)], load_sem.at[2]),
        near(qr_hbm, qr, load_sem.at[3]),
        near(q_hbm, qx.at[:, pl.ds(0, wid)], load_sem.at[4]),
        near(og_hbm, og, load_sem.at[5]),
        near(in_hbm, inp.at[0], load_sem.at[6]),
    ]
    for copy in loads:
        copy.start()

    n_rope = rope.shape[0]
    loads[0].wait()
    loads[1].wait()
    ids = doc[...]
    lane_t = iota((EXT, tok), 0)
    here_t = (lane_t - n_rope == ids).astype(F32).astype(BF16)
    tag_rows = (lane_t >= n_rope) & (lane_t < n_rope + 8)
    away_t = jnp.where(tag_rows & (lane_t - n_rope != ids), FAR, 0.0).astype(BF16)
    eye = (iota((tok, tok), 0) == iota((tok, tok), 1)).astype(F32).astype(BF16)
    here = dot(eye, here_t, NT).astype(BF16)
    tagged = jnp.concatenate([rope[...].astype(F32), away_t[n_rope:].astype(F32)], axis=0).astype(BF16)
    keys[pl.ds(own, tok), pl.ds(wid, EXT)] = dot(eye, tagged, NT).astype(BF16)
    loads[2].wait()

    pl.semaphore_wait(barrier, count)
    core = lax.rem(c, 2)
    side = pl.multiple_of((2 - 2 * core) * tok, tok)
    halo = [
        send(keys.at[pl.ds(own, tok)], keys.at[pl.ds(tok, tok)], hs_sem.at[0], hr_sem.at[0], ctx_at(2), h),
        send(keys.at[pl.ds(own, tok)], keys.at[pl.ds(side, tok)], hs_sem.at[1], hr_sem.at[1], ctx_at(1 + 2 * core), h),
    ]

    step = min(rows, 128)
    per = step // heads
    cols = heads * n_rope
    spread = (lax.div(iota((step, per), 0), heads) == iota((step, per), 1)).astype(F32).astype(BF16)
    gather = (lax.div(iota((per, step), 1), heads) == iota((per, step), 0)).astype(F32).astype(BF16)
    head_of = (lax.div(iota((step, cols), 1), n_rope) == lax.rem(iota((step, cols), 0), heads)).astype(F32)
    hot[...] = here
    pick[...] = (lax.rem(iota((cols, EXT), 0), n_rope) == iota((cols, EXT), 1)).astype(F32).astype(BF16)
    drop[...] = (lax.rem(iota((EXT, cols), 1), n_rope) == iota((EXT, cols), 0)).astype(F32).astype(BF16)
    line, place_of = iota((wid, wid), 0), iota((wid, wid), 1)
    target = lax.rem(lax.div(line, 8), n_z) * (8 * QUAD) + lax.div(line, 8 * n_z) * 8 + lax.rem(line, 8)
    perm[...] = (target == place_of).astype(F32).astype(BF16)
    loads[3].wait()

    @pl.loop(0, rows // step)
    def _(i):
        ts = pl.ds(pl.multiple_of(i * per, per), per)
        rs = pl.ds(pl.multiple_of(i * step, step), step)
        wide = (dot(spread, qr[ts, :]) * head_of).astype(BF16)
        qx[rs, pl.ds(wid, EXT)] = (dot(wide, pick[...]) + dot(spread, hot[ts, :])).astype(BF16)

    loads[4].wait()
    loads[5].wait()
    big = min(rows, 256)

    @pl.loop(0, rows // big)
    def _(i):
        rs = pl.ds(pl.multiple_of(i * big, big), big)
        low = pl.ds(pl.multiple_of(i * big + rows, big), big)
        both[rs, pl.ds(0, wid)] = dot(qx[rs, pl.ds(0, wid)], perm[...], NT).astype(BF16)
        both[rs, pl.ds(wid, EXT)] = qx[rs, pl.ds(wid, EXT)]
        both[low, pl.ds(0, wid)] = dot(og[rs, :], perm[...], NT).astype(BF16)

    def score(k0, k1, rs):
        st[pl.ds(k0, k1 - k0), rs] = dot(keys[pl.ds(k0, k1 - k0), :], qx[rs, :], NT)
        dt[pl.ds(k0, k1 - k0), rs] = dot(keys[pl.ds(k0, k1 - k0), pl.ds(0, wid)], og[rs, :], NT)

    @pl.loop(0, rows // big)
    def _(i):
        score(own, own + tok, pl.ds(pl.multiple_of(i * big, big), big))

    halo[0].wait_recv()
    across = pl.multiple_of(2 * core * tok, tok)
    halo.append(
        send(keys.at[pl.ds(tok, tok)], keys.at[pl.ds(across, tok)], hs_sem.at[2], hr_sem.at[2], ctx_at(1 - 2 * core), h))
    loads[6].wait()
    for copy in halo[1:]:
        copy.wait_recv()
    swap = [send(inp.at[0], inp.at[d], is_sem.at[d - 1], ir_sem.at[d - 1], quad_at(d), h) for d in (1, 2, 3)]
    def soft(i):
        rs = pl.ds(i * step, step)
        row = iota((tok, step), 0)
        t = i * per + lax.div(iota((tok, step), 1), heads)
        first = jnp.where(row > t, st[pl.ds(0, tok), rs], FAR)
        last = jnp.where(row <= t, st[pl.ds(own, tok), rs], FAR)
        s = jnp.concatenate([first, st[pl.ds(tok, own - tok), rs], last], axis=0)
        e = jnp.exp((s - jnp.max(s, axis=0, keepdims=True)) * SCALE)
        p = e * (1.0 / jnp.sum(e, axis=0, keepdims=True))
        low = p.astype(BF16)
        dp = dt[:, rs]
        delta = jnp.sum(low.astype(F32) * dp, axis=0, keepdims=True)
        weights[:, pl.ds(rows + i * step, step)] = low
        weights[:, rs] = (p * (dp - delta) * SCALE).astype(BF16)

    parts = big // step
    for i in range(rows // big + 1):
        if i < rows // big:
            score(0, own, pl.ds(i * big, big))
        if i:
            for m in range(parts):
                soft((i - 1) * parts + m)

    for k, (c0, cc) in enumerate(chunks):
        at = pl.ds(c0, cc)
        deep = pl.ds(0, 2 * rows if c0 < wid else rows)
        total = dot(weights[:, deep], both[deep, at])
        total = total.astype(BF16).reshape(SLOTS, n_x, tok // n_x, cc)
        for xi in range(n_x):
            part[xi, :, :, at] = total[:, xi]
        for d in range(1, n_x):
            send(part.at[x_at(d), :, :, at], xbuf.at[d - 1, :, :, at], xs_sem, xr_sem.at[k],
                 c, yh * n_x + x_at(d))

    def query_grads(i):
        ts = pl.ds(pl.multiple_of(i * per, per), per)
        rs = pl.ds(pl.multiple_of(i * step, step), step)
        g = dot(weights[:, rs], keys[...], TN)
        dq[rs, :] = g[:, :wid].astype(BF16)
        wide = (dot(g[:, wid:].astype(BF16), drop[...]) * head_of).astype(BF16)
        dqr[ts, :] = dot(gather, wide).astype(BF16)

    early = rows // step * 5 // 8
    pl.loop(0, early)(query_grads)

    for k, (c0, cc) in enumerate(chunks):
        at = pl.ds(c0, cc)
        group(xbuf.at[:, :, :, at], xs_sem, xr_sem.at[k]).wait_recv()
        total = part[x, :, :, at].astype(F32)
        for d in range(1, n_x):
            total = total + xbuf[d - 1, :, :, at].astype(F32)
        total = total.reshape(SLOTS, n_yh, 8, cc).astype(BF16)
        for yi in range(n_yh):
            ysend[yi, :, :, at] = total[:, yi]
        for s in range(SLOTS):
            for e in range(n_yh):
                if s < SLOTS - 1 or e:
                    send(ysend.at[yh_at(e), s, :, at], ybuf.at[(s * n_yh + e + n_yh) % y_n, :, at], ys_sem, yr_sem.at[k],
                         ctx_at(s - 3), yh_at(e) * n_x + x)

    pl.loop(early, rows // step)(query_grads)
    place_here = x * n_yh + yh
    def settle(k):
        at = pl.ds(*chunks[k])
        group(ybuf.at[pl.ds(1, y_n - 1), :, at], ys_sem, yr_sem.at[k]).wait_recv()
        total = ysend[yh, SLOTS - 1, :, at].astype(F32)
        total = total + jnp.sum(ybuf[pl.ds(1, y_n - 1), :, at].astype(F32), axis=0)
        gbuf[place_here, :, at] = total.astype(BF16)

    def spread_out(k):
        at = pl.ds(*chunks[k])
        for d in range(n_x):
            for e in range(n_yh):
                if d or e:
                    send(gbuf.at[place_here, :, at], gbuf.at[place_here, :, at], gs_sem, gr_sem.at[k],
                         c, yh_at(e) * n_x + x_at(d))

    quarter = wid // QUAD
    for k in (0, 1):
        settle(k)
        for to in (2 * k, 2 * k + 1):
            piece = gbuf.at[place_here, :, pl.ds(to * quarter, quarter)]
            by = lax.rem(to + QUAD - quad, QUAD)
            spot = tbuf.at[by * n_head + place_here]
            for d in reversed(range(n_x)):
                for e in reversed(range(n_yh)):
                    if d or e:
                        send(piece, spot, ts_sem, tr_sem, z * QUAD + to, yh_at(e) * n_x + x_at(d))

            @pl.when(quad != to)
            def _():
                send(piece, spot, ts_sem, tr_sem, z * QUAD + to, h)

            @pl.when(quad == to)
            def _():
                tbuf[place_here] = gbuf[place_here, :, pl.ds(to * quarter, quarter)]

    spread_out(0)
    spread_out(1)
    settle(2)
    spread_out(2)
    for copy in swap:
        copy.wait_recv()
    t_all = tbuf.at[pl.ds(0, QUAD * n_head - 1)]
    group(t_all, ts_sem, tr_sem).wait_recv()
    square = tbuf[...].astype(F32).reshape(QUAD * tok, quarter).astype(BF16)
    turned = dot((iota((quarter, quarter), 0) == iota((quarter, quarter), 1)).astype(F32).astype(BF16), square, NT)
    turned = turned.astype(BF16)
    total = dot(turned[:, :tok], inp[0], NT)
    for d in (1, 2, 3):
        total = total + dot(turned[:, d * tok:(d + 1) * tok], inp[d], NT)
    zsend[...] = total.reshape(n_z, 8, total.shape[1]).astype(BF16)
    for d in sorted(range(1, n_z), key=lambda d: -min(d, n_z - d)):
        send(zsend.at[lax.rem(z + d, n_z)], zbuf.at[d - 1], zs_sem, zr_sem, z_at(d), h)
    for k in range(3):
        group(gbuf.at[pl.ds(0, n_head - 1), :, pl.ds(*chunks[k])], gs_sem, gr_sem.at[k]).wait_recv()
    whole = gbuf[...].astype(F32).reshape(tok, full).astype(BF16)
    lg_out[...] = dot(whole[:, :wid], perm[...]).astype(BF16)
    take = (iota((n_rope, EXT), 0) == iota((n_rope, EXT), 1)).astype(F32).astype(BF16)
    krx[...] = dot(take, whole[:, wid:], NT).astype(BF16)
    total = zsend[z].astype(F32)
    for k, (c0, cc) in enumerate(chunks):
        at = pl.ds(c0, cc)
        group(xbuf.at[:, :, :, at], xs_sem, xr_sem.at[k]).wait_send()
        group(ybuf.at[pl.ds(1, y_n - 1), :, at], ys_sem, yr_sem.at[k]).wait_send()
        group(gbuf.at[pl.ds(0, n_head - 1), :, at], gs_sem, gr_sem.at[k]).wait_send()
    group(t_all, ts_sem, tr_sem).wait_send()
    for copy in halo + swap:
        copy.wait_send()
    group(zbuf, zs_sem, zr_sem).wait_recv()
    total = total + jnp.sum(zbuf[...].astype(F32), axis=0)
    pg_out[...] = total
    group(zbuf, zs_sem, zr_sem).wait_send()


def flush(*refs):
    sem = refs[-1]
    copies = [pltpu.make_async_copy(refs[i], refs[i + 5], sem.at[i]) for i in range(5)]
    for copy in copies:
        copy.start()
    for copy in copies:
        copy.wait()


def solution(mesh):
    n_ctx, n_head = mesh.shape["ctx"], mesh.shape["head"]
    n_x = 4 if n_head == 16 else 2
    n_yh = n_head // n_x
    n_z = n_ctx // QUAD

    def shards(q_latent, q_rope, latent, key_rope, out_grad, inputs, doc_ids):
        tok, heads, wid = q_latent.shape
        n_rope, dloc = key_rope.shape[1], inputs.shape[1]
        rows, full, keys = tok * heads, wid + EXT, SLOTS * tok
        cfg = (n_ctx, n_z, n_yh, n_x, tok, wid, heads)
        vm = pltpu.VMEM
        dma = pltpu.SemaphoreType.DMA
        y_n = SLOTS * n_yh
        shape = jax.ShapeDtypeStruct
        anywhere, local = pl.BlockSpec(memory_space=pltpu.HBM), pl.BlockSpec(memory_space=pltpu.VMEM)
        shapes = (
                shape((rows, wid), BF16),
                shape((tok, heads * n_rope), BF16),
                shape((tok, wid), BF16),
                shape((n_rope, tok), BF16),
                shape((8, dloc), F32),
            )
        outs = pl.pallas_call(
            functools.partial(kernel, cfg),
            out_shape=shapes,
            in_specs=[pl.BlockSpec(memory_space=pltpu.HBM)] * 7,
            out_specs=(local,) * 5,
            scratch_shapes=[
                vm((rows, full), BF16), vm((rows, wid), BF16), vm((tok, heads * n_rope), BF16),
                vm((keys, full), BF16), vm((n_rope, tok), BF16), vm((QUAD, dloc, tok), BF16),
                vm((1, tok), jnp.int32), vm((wid, wid), BF16),
                vm((keys, rows), F32), vm((keys, rows), F32), vm((keys, 2 * rows), BF16), vm((2 * rows, full), BF16),
                vm((n_x, SLOTS, tok // n_x, full), BF16), vm((n_x - 1, SLOTS, tok // n_x, full), BF16),
                vm((n_yh, SLOTS, 8, full), BF16), vm((y_n, 8, full), BF16),
                vm((n_head, 8, full), BF16), vm((QUAD * n_head, 8, wid // QUAD), BF16),
                vm((n_z, 8, dloc), BF16), vm((n_z - 1, 8, dloc), BF16),
                vm((tok, EXT), BF16), vm((heads * n_rope, EXT), BF16), vm((EXT, heads * n_rope), BF16),
                dma((7,)), dma((3,)), dma((3,)), dma, dma((3,)), dma, dma((3,)), dma, dma((3,)),
                dma, dma, dma((3,)), dma((3,)), dma, dma,
            ],
            compiler_params=pltpu.CompilerParams(collective_id=0, has_side_effects=True, vmem_limit_bytes=54_000_000),
            name="step",
        )(
            q_latent.reshape(rows, wid), q_rope, latent, key_rope.T, out_grad.reshape(rows, wid), inputs.T,
            doc_ids.reshape(n_ctx, 1, tok),
        )
        outs = pl.pallas_call(
            flush,
            out_shape=shapes,
            in_specs=[local] * 5,
            out_specs=(anywhere,) * 5,
            scratch_shapes=[dma((5,))],
            compiler_params=pltpu.CompilerParams(vmem_limit_bytes=2 << 20),
            name="flush",
        )(*outs)
        return (outs[0].reshape(tok, heads, wid), outs[1], outs[2], outs[3].T, outs[4])

    return jax.shard_map(
        shards,
        mesh=mesh,
        in_specs=(P("ctx", "head", None), P("ctx", "head"), P("ctx", None), P("ctx", None), P("ctx", "head", None),
                  P("ctx", "head"), P()),
        out_specs=(P("ctx", "head", None), P("ctx", "head"), P("ctx", None), P("ctx", None), P("ctx", "head")),
        check_vma=False,
    )
```

```python
import functools

import jax
import jax.numpy as jnp
from jax import lax
from jax.experimental import pallas as pl
from jax.experimental.pallas import tpu as pltpu
from jax.sharding import PartitionSpec as P

MESH = pl.DeviceIdType.MESH
BF16, F32 = jnp.bfloat16, jnp.float32
SCALE = 192.0 ** (-0.5)
FAR = -1e30
EXT = 128
QUAD = 4
SLOTS = 4
NT = (((1,), (1,)), ((), ()))
TN = (((0,), (0,)), ((), ()))


def dot(a, b, dims=(((1,), (0,)), ((), ()))):
    return lax.dot_general(a, b, dims, preferred_element_type=F32)


def iota(shape, dim):
    return lax.broadcasted_iota(jnp.int32, shape, dim)


def kernel(cfg, q_hbm, qr_hbm, lat_hbm, rope_hbm, og_hbm, in_hbm, doc_hbm,
           dq, dqr, lg_out, krx, pg_out,
           qx, og, qr, keys, rope, inp, doc, perm, st, dt, weights, both, part, xbuf, ysend, ybuf,
           gbuf, tbuf, zsend, zbuf, hot, pick, drop,
           load_sem, hs_sem, hr_sem, xs_sem, xr_sem, ys_sem, yr_sem, gs_sem, gr_sem,
           ts_sem, tr_sem, is_sem, ir_sem, zs_sem, zr_sem):
    n_ctx, n_z, n_yh, n_x, tok, wid, heads = cfg
    rows = tok * heads
    n_head = n_yh * n_x
    full = wid + EXT
    c, h = lax.axis_index("ctx"), lax.axis_index("head")
    z, quad = lax.div(c, QUAD), lax.rem(c, QUAD)
    yh, x = lax.div(h, n_x), lax.rem(h, n_x)
    own = (SLOTS - 1) * tok
    y_n = SLOTS * n_yh
    chunks = [(0, wid // 2), (wid // 2, wid // 2), (wid, EXT)]

    def ctx_at(by):
        return lax.rem(c + (by + n_ctx), n_ctx)

    def yh_at(by):
        return lax.rem(yh + by, n_yh)

    def x_at(by):
        return lax.rem(x + by, n_x)

    def quad_at(by):
        return z * QUAD + lax.rem(quad + by, QUAD)

    def z_at(by):
        return lax.rem(z + by, n_z) * QUAD + quad

    def near(ref_a, ref_b, sem):
        return pltpu.make_async_copy(ref_a, ref_b, sem)

    def send(src, dst, ssem, rsem, ci, hi):
        copy = pltpu.make_async_remote_copy(
            src_ref=src, dst_ref=dst, send_sem=ssem, recv_sem=rsem, device_id=(ci, hi), device_id_type=MESH
        )
        copy.start()
        return copy

    def group(ref, ssem, rsem):
        return pltpu.make_async_remote_copy(
            src_ref=ref, dst_ref=ref, send_sem=ssem, recv_sem=rsem, device_id=(c, h), device_id_type=MESH
        )

    loads = [
        near(doc_hbm.at[c], doc, load_sem.at[0]),
        near(rope_hbm, rope, load_sem.at[1]),
        near(lat_hbm, keys.at[pl.ds(own, tok), pl.ds(0, wid)], load_sem.at[2]),
        near(qr_hbm, qr, load_sem.at[3]),
        near(q_hbm, qx.at[:, pl.ds(0, wid)], load_sem.at[4]),
        near(og_hbm, og, load_sem.at[5]),
        near(in_hbm, inp.at[0], load_sem.at[6]),
    ]
    for copy in loads:
        copy.start()

    barrier = pltpu.get_barrier_semaphore()
    count = 0
    for by in range(-3, 4):
        for e in range(n_yh):
            if by or e:
                pl.semaphore_signal(barrier, inc=1, device_id=(ctx_at(by), yh_at(e) * n_x + x), device_id_type=MESH)
                count += 1
    for d in range(1, n_x):
        for e in range(n_yh):
            pl.semaphore_signal(barrier, inc=1, device_id=(c, yh_at(e) * n_x + x_at(d)), device_id_type=MESH)
            count += 1
    for by in range(1, QUAD):
        for d in range(1, n_x):
            for e in range(n_yh):
                pl.semaphore_signal(
                    barrier, inc=1, device_id=(quad_at(by), yh_at(e) * n_x + x_at(d)), device_id_type=MESH)
                count += 1
    for d in range(1, n_z):
        pl.semaphore_signal(barrier, inc=1, device_id=(z_at(d), h), device_id_type=MESH)
        count += 1

    n_rope = rope.shape[0]
    loads[0].wait()
    loads[1].wait()
    ids = doc[...]
    lane_t = iota((EXT, tok), 0)
    here_t = (lane_t - n_rope == ids).astype(F32).astype(BF16)
    tag_rows = (lane_t >= n_rope) & (lane_t < n_rope + 8)
    away_t = jnp.where(tag_rows & (lane_t - n_rope != ids), FAR, 0.0).astype(BF16)
    eye = (iota((tok, tok), 0) == iota((tok, tok), 1)).astype(F32).astype(BF16)
    here = dot(eye, here_t, NT).astype(BF16)
    tagged = jnp.concatenate([rope[...].astype(F32), away_t[n_rope:].astype(F32)], axis=0).astype(BF16)
    keys[pl.ds(own, tok), pl.ds(wid, EXT)] = dot(eye, tagged, NT).astype(BF16)
    loads[2].wait()

    pl.semaphore_wait(barrier, count)
    core = lax.rem(c, 2)
    side = pl.multiple_of((2 - 2 * core) * tok, tok)
    halo = [
        send(keys.at[pl.ds(own, tok)], keys.at[pl.ds(tok, tok)], hs_sem.at[0], hr_sem.at[0], ctx_at(2), h),
        send(keys.at[pl.ds(own, tok)], keys.at[pl.ds(side, tok)], hs_sem.at[1], hr_sem.at[1], ctx_at(1 + 2 * core), h),
    ]

    step = min(rows, 128)
    per = step // heads
    cols = heads * n_rope
    spread = (lax.div(iota((step, per), 0), heads) == iota((step, per), 1)).astype(F32).astype(BF16)
    gather = (lax.div(iota((per, step), 1), heads) == iota((per, step), 0)).astype(F32).astype(BF16)
    head_of = (lax.div(iota((step, cols), 1), n_rope) == lax.rem(iota((step, cols), 0), heads)).astype(F32)
    hot[...] = here
    pick[...] = (lax.rem(iota((cols, EXT), 0), n_rope) == iota((cols, EXT), 1)).astype(F32).astype(BF16)
    drop[...] = (lax.rem(iota((EXT, cols), 1), n_rope) == iota((EXT, cols), 0)).astype(F32).astype(BF16)
    line, place_of = iota((wid, wid), 0), iota((wid, wid), 1)
    target = lax.rem(lax.div(line, 8), n_z) * (8 * QUAD) + lax.div(line, 8 * n_z) * 8 + lax.rem(line, 8)
    perm[...] = (target == place_of).astype(F32).astype(BF16)
    loads[3].wait()

    @pl.loop(0, rows // step)
    def _(i):
        ts = pl.ds(pl.multiple_of(i * per, per), per)
        rs = pl.ds(pl.multiple_of(i * step, step), step)
        wide = (dot(spread, qr[ts, :]) * head_of).astype(BF16)
        qx[rs, pl.ds(wid, EXT)] = (dot(wide, pick[...]) + dot(spread, hot[ts, :])).astype(BF16)

    loads[4].wait()
    loads[5].wait()
    big = min(rows, 256)

    def score(k0, k1, rs):
        st[pl.ds(k0, k1 - k0), rs] = dot(keys[pl.ds(k0, k1 - k0), :], qx[rs, :], NT)
        dt[pl.ds(k0, k1 - k0), rs] = dot(keys[pl.ds(k0, k1 - k0), pl.ds(0, wid)], og[rs, :], NT)

    @pl.loop(0, rows // big)
    def _(i):
        score(own, own + tok, pl.ds(pl.multiple_of(i * big, big), big))

    halo[0].wait_recv()
    across = pl.multiple_of(2 * core * tok, tok)
    halo.append(
        send(keys.at[pl.ds(tok, tok)], keys.at[pl.ds(across, tok)], hs_sem.at[2], hr_sem.at[2], ctx_at(1 - 2 * core), h))
    @pl.loop(0, rows // big)
    def _(i):
        rs = pl.ds(pl.multiple_of(i * big, big), big)
        low = pl.ds(pl.multiple_of(i * big + rows, big), big)
        both[rs, pl.ds(0, wid)] = dot(qx[rs, pl.ds(0, wid)], perm[...], NT).astype(BF16)
        both[rs, pl.ds(wid, EXT)] = qx[rs, pl.ds(wid, EXT)]
        both[low, pl.ds(0, wid)] = dot(og[rs, :], perm[...], NT).astype(BF16)

    loads[6].wait()
    for copy in halo[1:]:
        copy.wait_recv()
    swap = [send(inp.at[0], inp.at[d], is_sem.at[d - 1], ir_sem.at[d - 1], quad_at(d), h) for d in (1, 2, 3)]
    def soft(i):
        rs = pl.ds(i * step, step)
        row = iota((tok, step), 0)
        t = i * per + lax.div(iota((tok, step), 1), heads)
        first = jnp.where(row > t, st[pl.ds(0, tok), rs], FAR)
        last = jnp.where(row <= t, st[pl.ds(own, tok), rs], FAR)
        s = jnp.concatenate([first, st[pl.ds(tok, own - tok), rs], last], axis=0)
        e = jnp.exp((s - jnp.max(s, axis=0, keepdims=True)) * SCALE)
        p = e * (1.0 / jnp.sum(e, axis=0, keepdims=True))
        low = p.astype(BF16)
        dp = dt[:, rs]
        delta = jnp.sum(low.astype(F32) * dp, axis=0, keepdims=True)
        weights[:, pl.ds(rows + i * step, step)] = low
        weights[:, rs] = (p * (dp - delta) * SCALE).astype(BF16)

    parts = big // step
    for i in range(rows // big + 1):
        if i < rows // big:
            score(0, own, pl.ds(i * big, big))
        if i:
            for m in range(parts):
                soft((i - 1) * parts + m)

    for k, (c0, cc) in enumerate(chunks):
        at = pl.ds(c0, cc)
        deep = pl.ds(0, 2 * rows if c0 < wid else rows)
        total = dot(weights[:, deep], both[deep, at])
        total = total.astype(BF16).reshape(SLOTS, n_x, tok // n_x, cc)
        for xi in range(n_x):
            part[xi, :, :, at] = total[:, xi]
        for d in range(1, n_x):
            send(part.at[x_at(d), :, :, at], xbuf.at[d - 1, :, :, at], xs_sem, xr_sem.at[k],
                 c, yh * n_x + x_at(d))

    def query_grads(i):
        ts = pl.ds(pl.multiple_of(i * per, per), per)
        rs = pl.ds(pl.multiple_of(i * step, step), step)
        g = dot(weights[:, rs], keys[...], TN)
        dq[rs, :] = g[:, :wid].astype(BF16)
        wide = (dot(g[:, wid:].astype(BF16), drop[...]) * head_of).astype(BF16)
        dqr[ts, :] = dot(gather, wide).astype(BF16)

    early = rows // step * 5 // 8
    pl.loop(0, early)(query_grads)

    for k, (c0, cc) in enumerate(chunks):
        at = pl.ds(c0, cc)
        group(xbuf.at[:, :, :, at], xs_sem, xr_sem.at[k]).wait_recv()
        total = part[x, :, :, at].astype(F32)
        for d in range(1, n_x):
            total = total + xbuf[d - 1, :, :, at].astype(F32)
        total = total.reshape(SLOTS, n_yh, 8, cc).astype(BF16)
        for yi in range(n_yh):
            ysend[yi, :, :, at] = total[:, yi]
        for s in range(SLOTS):
            for e in range(n_yh):
                if s < SLOTS - 1 or e:
                    send(ysend.at[yh_at(e), s, :, at], ybuf.at[(s * n_yh + e + n_yh) % y_n, :, at], ys_sem, yr_sem.at[k],
                         ctx_at(s - 3), yh_at(e) * n_x + x)

    pl.loop(early, rows // step)(query_grads)
    place_here = x * n_yh + yh
    def settle(k):
        at = pl.ds(*chunks[k])
        group(ybuf.at[pl.ds(1, y_n - 1), :, at], ys_sem, yr_sem.at[k]).wait_recv()
        total = ysend[yh, SLOTS - 1, :, at].astype(F32)
        total = total + jnp.sum(ybuf[pl.ds(1, y_n - 1), :, at].astype(F32), axis=0)
        gbuf[place_here, :, at] = total.astype(BF16)

    def spread_out(k):
        at = pl.ds(*chunks[k])
        for d in range(n_x):
            for e in range(n_yh):
                if d or e:
                    send(gbuf.at[place_here, :, at], gbuf.at[place_here, :, at], gs_sem, gr_sem.at[k],
                         c, yh_at(e) * n_x + x_at(d))

    quarter = wid // QUAD
    for k in (0, 1):
        settle(k)
        for to in (2 * k, 2 * k + 1):
            piece = gbuf.at[place_here, :, pl.ds(to * quarter, quarter)]
            by = lax.rem(to + QUAD - quad, QUAD)
            spot = tbuf.at[by * n_head + place_here]
            for d in reversed(range(n_x)):
                for e in reversed(range(n_yh)):
                    if d or e:
                        send(piece, spot, ts_sem, tr_sem, z * QUAD + to, yh_at(e) * n_x + x_at(d))

            @pl.when(quad != to)
            def _():
                send(piece, spot, ts_sem, tr_sem, z * QUAD + to, h)

            @pl.when(quad == to)
            def _():
                tbuf[place_here] = gbuf[place_here, :, pl.ds(to * quarter, quarter)]

    spread_out(0)
    spread_out(1)
    settle(2)
    spread_out(2)
    for copy in swap:
        copy.wait_recv()
    t_all = tbuf.at[pl.ds(0, QUAD * n_head - 1)]
    group(t_all, ts_sem, tr_sem).wait_recv()
    square = tbuf[...].astype(F32).reshape(QUAD * tok, quarter).astype(BF16)
    turned = dot((iota((quarter, quarter), 0) == iota((quarter, quarter), 1)).astype(F32).astype(BF16), square, NT)
    turned = turned.astype(BF16)
    total = dot(turned[:, :tok], inp[0], NT)
    for d in (1, 2, 3):
        total = total + dot(turned[:, d * tok:(d + 1) * tok], inp[d], NT)
    zsend[...] = total.reshape(n_z, 8, total.shape[1]).astype(BF16)
    for d in sorted(range(1, n_z), key=lambda d: -min(d, n_z - d)):
        send(zsend.at[lax.rem(z + d, n_z)], zbuf.at[d - 1], zs_sem, zr_sem, z_at(d), h)
    for k in range(3):
        group(gbuf.at[pl.ds(0, n_head - 1), :, pl.ds(*chunks[k])], gs_sem, gr_sem.at[k]).wait_recv()
    whole = gbuf[...].astype(F32).reshape(tok, full).astype(BF16)
    lg_out[...] = dot(whole[:, :wid], perm[...]).astype(BF16)
    take = (iota((n_rope, EXT), 0) == iota((n_rope, EXT), 1)).astype(F32).astype(BF16)
    krx[...] = dot(take, whole[:, wid:], NT).astype(BF16)
    total = zsend[z].astype(F32)
    for k, (c0, cc) in enumerate(chunks):
        at = pl.ds(c0, cc)
        group(xbuf.at[:, :, :, at], xs_sem, xr_sem.at[k]).wait_send()
        group(ybuf.at[pl.ds(1, y_n - 1), :, at], ys_sem, yr_sem.at[k]).wait_send()
        group(gbuf.at[pl.ds(0, n_head - 1), :, at], gs_sem, gr_sem.at[k]).wait_send()
    group(t_all, ts_sem, tr_sem).wait_send()
    for copy in halo + swap:
        copy.wait_send()
    group(zbuf, zs_sem, zr_sem).wait_recv()
    total = total + jnp.sum(zbuf[...].astype(F32), axis=0)
    pg_out[...] = total
    group(zbuf, zs_sem, zr_sem).wait_send()


def flush(*refs):
    sem = refs[-1]
    copies = [pltpu.make_async_copy(refs[i], refs[i + 5], sem.at[i]) for i in range(5)]
    for copy in copies:
        copy.start()
    for copy in copies:
        copy.wait()


def solution(mesh):
    n_ctx, n_head = mesh.shape["ctx"], mesh.shape["head"]
    n_x = 4 if n_head == 16 else 2
    n_yh = n_head // n_x
    n_z = n_ctx // QUAD

    def shards(q_latent, q_rope, latent, key_rope, out_grad, inputs, doc_ids):
        tok, heads, wid = q_latent.shape
        n_rope, dloc = key_rope.shape[1], inputs.shape[1]
        rows, full, keys = tok * heads, wid + EXT, SLOTS * tok
        cfg = (n_ctx, n_z, n_yh, n_x, tok, wid, heads)
        vm = pltpu.VMEM
        dma = pltpu.SemaphoreType.DMA
        y_n = SLOTS * n_yh
        shape = jax.ShapeDtypeStruct
        anywhere, local = pl.BlockSpec(memory_space=pltpu.HBM), pl.BlockSpec(memory_space=pltpu.VMEM)
        shapes = (
                shape((rows, wid), BF16),
                shape((tok, heads * n_rope), BF16),
                shape((tok, wid), BF16),
                shape((n_rope, tok), BF16),
                shape((8, dloc), F32),
            )
        outs = pl.pallas_call(
            functools.partial(kernel, cfg),
            out_shape=shapes,
            in_specs=[pl.BlockSpec(memory_space=pltpu.HBM)] * 7,
            out_specs=(local,) * 5,
            scratch_shapes=[
                vm((rows, full), BF16), vm((rows, wid), BF16), vm((tok, heads * n_rope), BF16),
                vm((keys, full), BF16), vm((n_rope, tok), BF16), vm((QUAD, dloc, tok), BF16),
                vm((1, tok), jnp.int32), vm((wid, wid), BF16),
                vm((keys, rows), F32), vm((keys, rows), F32), vm((keys, 2 * rows), BF16), vm((2 * rows, full), BF16),
                vm((n_x, SLOTS, tok // n_x, full), BF16), vm((n_x - 1, SLOTS, tok // n_x, full), BF16),
                vm((n_yh, SLOTS, 8, full), BF16), vm((y_n, 8, full), BF16),
                vm((n_head, 8, full), BF16), vm((QUAD * n_head, 8, wid // QUAD), BF16),
                vm((n_z, 8, dloc), BF16), vm((n_z - 1, 8, dloc), BF16),
                vm((tok, EXT), BF16), vm((heads * n_rope, EXT), BF16), vm((EXT, heads * n_rope), BF16),
                dma((7,)), dma((3,)), dma((3,)), dma, dma((3,)), dma, dma((3,)), dma, dma((3,)),
                dma, dma, dma((3,)), dma((3,)), dma, dma,
            ],
            compiler_params=pltpu.CompilerParams(collective_id=0, has_side_effects=True, vmem_limit_bytes=48 << 20),
            name="step",
        )(*(
            pltpu.with_memory_space_constraint(a, pltpu.HBM)
            for a in (q_latent.reshape(rows, wid), q_rope, latent, key_rope.T, out_grad.reshape(rows, wid), inputs.T,
                      doc_ids.reshape(n_ctx, 1, tok))
        ))
        outs = pl.pallas_call(
            flush,
            out_shape=shapes,
            in_specs=[local] * 5,
            out_specs=(anywhere,) * 5,
            scratch_shapes=[dma((5,))],
            compiler_params=pltpu.CompilerParams(vmem_limit_bytes=2 << 20),
            name="flush",
        )(*outs)
        return (outs[0].reshape(tok, heads, wid), outs[1], outs[2], outs[3].T, outs[4])

    return jax.shard_map(
        shards,
        mesh=mesh,
        in_specs=(P("ctx", "head", None), P("ctx", "head"), P("ctx", None), P("ctx", None), P("ctx", "head", None),
                  P("ctx", "head"), P()),
        out_specs=(P("ctx", "head", None), P("ctx", "head"), P("ctx", None), P("ctx", None), P("ctx", "head")),
        check_vma=False,
    )
```

```python
import functools

import jax
import jax.numpy as jnp
from jax import lax
from jax.experimental import pallas as pl
from jax.experimental.pallas import tpu as pltpu
from jax.sharding import PartitionSpec as P

MESH = pl.DeviceIdType.MESH
BF16, F32 = jnp.bfloat16, jnp.float32
SCALE = 192.0 ** (-0.5)
FAR = -1e30
EXT = 128
QUAD = 4
SLOTS = 4
NT = (((1,), (1,)), ((), ()))
TN = (((0,), (0,)), ((), ()))


def dot(a, b, dims=(((1,), (0,)), ((), ()))):
    return lax.dot_general(a, b, dims, preferred_element_type=F32)


def iota(shape, dim):
    return lax.broadcasted_iota(jnp.int32, shape, dim)


def kernel(cfg, q_hbm, qr_hbm, lat_hbm, rope_hbm, og_hbm, in_hbm, doc_hbm,
           dq, dqr, lg_out, krx, pg_out,
           qx, og, qr, keys, rope, inp, doc, perm, st, dt, weights, both, part, xbuf, ysend, ybuf,
           gbuf, tbuf, zsend, zbuf, hot, pick, drop,
           load_sem, hs_sem, hr_sem, xs_sem, xr_sem, ys_sem, yr_sem, gs_sem, gr_sem,
           ts_sem, tr_sem, is_sem, ir_sem, zs_sem, zr_sem):
    n_ctx, n_z, n_yh, n_x, tok, wid, heads = cfg
    rows = tok * heads
    n_head = n_yh * n_x
    full = wid + EXT
    c, h = lax.axis_index("ctx"), lax.axis_index("head")
    z, quad = lax.div(c, QUAD), lax.rem(c, QUAD)
    yh, x = lax.div(h, n_x), lax.rem(h, n_x)
    own = (SLOTS - 1) * tok
    y_n = SLOTS * n_yh
    chunks = [(0, wid // 2), (wid // 2, wid // 2), (wid, EXT)]

    def ctx_at(by):
        return lax.rem(c + (by + n_ctx), n_ctx)

    def yh_at(by):
        return lax.rem(yh + by, n_yh)

    def x_at(by):
        return lax.rem(x + by, n_x)

    def quad_at(by):
        return z * QUAD + lax.rem(quad + by, QUAD)

    def z_at(by):
        return lax.rem(z + by, n_z) * QUAD + quad

    def near(ref_a, ref_b, sem):
        return pltpu.make_async_copy(ref_a, ref_b, sem)

    def send(src, dst, ssem, rsem, ci, hi):
        copy = pltpu.make_async_remote_copy(
            src_ref=src, dst_ref=dst, send_sem=ssem, recv_sem=rsem, device_id=(ci, hi), device_id_type=MESH
        )
        copy.start()
        return copy

    def group(ref, ssem, rsem):
        return pltpu.make_async_remote_copy(
            src_ref=ref, dst_ref=ref, send_sem=ssem, recv_sem=rsem, device_id=(c, h), device_id_type=MESH
        )

    loads = [
        near(doc_hbm.at[c], doc, load_sem.at[0]),
        near(rope_hbm, rope, load_sem.at[1]),
        near(lat_hbm, keys.at[pl.ds(own, tok), pl.ds(0, wid)], load_sem.at[2]),
        near(qr_hbm, qr, load_sem.at[3]),
        near(q_hbm, qx.at[:, pl.ds(0, wid)], load_sem.at[4]),
        near(og_hbm, og, load_sem.at[5]),
        near(in_hbm, inp.at[0], load_sem.at[6]),
    ]
    for copy in loads:
        copy.start()

    barrier = pltpu.get_barrier_semaphore()
    count = 0
    for by in range(-3, 4):
        for e in range(n_yh):
            if by or e:
                pl.semaphore_signal(barrier, inc=1, device_id=(ctx_at(by), yh_at(e) * n_x + x), device_id_type=MESH)
                count += 1
    for d in range(1, n_x):
        for e in range(n_yh):
            pl.semaphore_signal(barrier, inc=1, device_id=(c, yh_at(e) * n_x + x_at(d)), device_id_type=MESH)
            count += 1
    for by in range(1, QUAD):
        for d in range(1, n_x):
            for e in range(n_yh):
                pl.semaphore_signal(
                    barrier, inc=1, device_id=(quad_at(by), yh_at(e) * n_x + x_at(d)), device_id_type=MESH)
                count += 1
    for d in range(1, n_z):
        pl.semaphore_signal(barrier, inc=1, device_id=(z_at(d), h), device_id_type=MESH)
        count += 1

    n_rope = rope.shape[0]
    loads[0].wait()
    loads[1].wait()
    ids = doc[...]
    lane_t = iota((EXT, tok), 0)
    here_t = (lane_t - n_rope == ids).astype(F32).astype(BF16)
    tag_rows = (lane_t >= n_rope) & (lane_t < n_rope + 8)
    away_t = jnp.where(tag_rows & (lane_t - n_rope != ids), FAR, 0.0).astype(BF16)
    eye = (iota((tok, tok), 0) == iota((tok, tok), 1)).astype(F32).astype(BF16)
    here = dot(eye, here_t, NT).astype(BF16)
    tagged = jnp.concatenate([rope[...].astype(F32), away_t[n_rope:].astype(F32)], axis=0).astype(BF16)
    keys[pl.ds(own, tok), pl.ds(wid, EXT)] = dot(eye, tagged, NT).astype(BF16)
    loads[2].wait()

    pl.semaphore_wait(barrier, count)
    core = lax.rem(c, 2)
    side = pl.multiple_of((2 - 2 * core) * tok, tok)
    halo = [
        send(keys.at[pl.ds(own, tok)], keys.at[pl.ds(tok, tok)], hs_sem.at[0], hr_sem.at[0], ctx_at(2), h),
        send(keys.at[pl.ds(own, tok)], keys.at[pl.ds(side, tok)], hs_sem.at[1], hr_sem.at[1], ctx_at(1 + 2 * core), h),
    ]

    step = min(rows, 128)
    per = step // heads
    cols = heads * n_rope
    spread = (lax.div(iota((step, per), 0), heads) == iota((step, per), 1)).astype(F32).astype(BF16)
    gather = (lax.div(iota((per, step), 1), heads) == iota((per, step), 0)).astype(F32).astype(BF16)
    head_of = (lax.div(iota((step, cols), 1), n_rope) == lax.rem(iota((step, cols), 0), heads)).astype(F32)
    hot[...] = here
    pick[...] = (lax.rem(iota((cols, EXT), 0), n_rope) == iota((cols, EXT), 1)).astype(F32).astype(BF16)
    drop[...] = (lax.rem(iota((EXT, cols), 1), n_rope) == iota((EXT, cols), 0)).astype(F32).astype(BF16)
    line, place_of = iota((wid, wid), 0), iota((wid, wid), 1)
    target = lax.rem(lax.div(line, 8), n_z) * (8 * QUAD) + lax.div(line, 8 * n_z) * 8 + lax.rem(line, 8)
    perm[...] = (target == place_of).astype(F32).astype(BF16)
    loads[3].wait()

    @pl.loop(0, rows // step)
    def _(i):
        ts = pl.ds(pl.multiple_of(i * per, per), per)
        rs = pl.ds(pl.multiple_of(i * step, step), step)
        wide = (dot(spread, qr[ts, :]) * head_of).astype(BF16)
        qx[rs, pl.ds(wid, EXT)] = (dot(wide, pick[...]) + dot(spread, hot[ts, :])).astype(BF16)

    loads[4].wait()
    loads[5].wait()
    big = min(rows, 256)

    def score(k0, k1, rs):
        st[pl.ds(k0, k1 - k0), rs] = dot(keys[pl.ds(k0, k1 - k0), :], qx[rs, :], NT)
        dt[pl.ds(k0, k1 - k0), rs] = dot(keys[pl.ds(k0, k1 - k0), pl.ds(0, wid)], og[rs, :], NT)

    @pl.loop(0, rows // big)
    def _(i):
        score(own, own + tok, pl.ds(pl.multiple_of(i * big, big), big))

    halo[0].wait_recv()
    across = pl.multiple_of(2 * core * tok, tok)
    halo.append(
        send(keys.at[pl.ds(tok, tok)], keys.at[pl.ds(across, tok)], hs_sem.at[2], hr_sem.at[2], ctx_at(1 - 2 * core), h))
    @pl.loop(0, rows // big)
    def _(i):
        rs = pl.ds(pl.multiple_of(i * big, big), big)
        low = pl.ds(pl.multiple_of(i * big + rows, big), big)
        both[rs, pl.ds(0, wid)] = dot(qx[rs, pl.ds(0, wid)], perm[...], NT).astype(BF16)
        both[rs, pl.ds(wid, EXT)] = qx[rs, pl.ds(wid, EXT)]
        both[low, pl.ds(0, wid)] = dot(og[rs, :], perm[...], NT).astype(BF16)

    loads[6].wait()
    for copy in halo[1:]:
        copy.wait_recv()
    swap = [send(inp.at[0], inp.at[d], is_sem.at[d - 1], ir_sem.at[d - 1], quad_at(d), h) for d in (1, 2, 3)]
    def soft(i):
        rs = pl.ds(i * step, step)
        row = iota((tok, step), 0)
        t = i * per + lax.div(iota((tok, step), 1), heads)
        first = jnp.where(row > t, st[pl.ds(0, tok), rs], FAR)
        last = jnp.where(row <= t, st[pl.ds(own, tok), rs], FAR)
        s = jnp.concatenate([first, st[pl.ds(tok, own - tok), rs], last], axis=0)
        e = jnp.exp((s - jnp.max(s, axis=0, keepdims=True)) * SCALE)
        p = e * (1.0 / jnp.sum(e, axis=0, keepdims=True))
        low = p.astype(BF16)
        dp = dt[:, rs]
        delta = jnp.sum(low.astype(F32) * dp, axis=0, keepdims=True)
        weights[:, pl.ds(rows + i * step, step)] = low
        weights[:, rs] = (p * (dp - delta) * SCALE).astype(BF16)

    parts = big // step
    for i in range(rows // big + 1):
        if i < rows // big:
            score(0, own, pl.ds(i * big, big))
        if i:
            for m in range(parts):
                soft((i - 1) * parts + m)

    for k, (c0, cc) in enumerate(chunks):
        at = pl.ds(c0, cc)
        deep = pl.ds(0, 2 * rows if c0 < wid else rows)
        total = dot(weights[:, deep], both[deep, at])
        total = total.astype(BF16).reshape(SLOTS, n_x, tok // n_x, cc)
        for xi in range(n_x):
            part[xi, :, :, at] = total[:, xi]
        for d in range(1, n_x):
            send(part.at[x_at(d), :, :, at], xbuf.at[d - 1, :, :, at], xs_sem, xr_sem.at[k],
                 c, yh * n_x + x_at(d))

    def query_grads(i):
        ts = pl.ds(pl.multiple_of(i * per, per), per)
        rs = pl.ds(pl.multiple_of(i * step, step), step)
        g = dot(weights[:, rs], keys[...], TN)
        dq[rs, :] = g[:, :wid].astype(BF16)
        wide = (dot(g[:, wid:].astype(BF16), drop[...]) * head_of).astype(BF16)
        dqr[ts, :] = dot(gather, wide).astype(BF16)


    for k, (c0, cc) in enumerate(chunks):
        at = pl.ds(c0, cc)
        group(xbuf.at[:, :, :, at], xs_sem, xr_sem.at[k]).wait_recv()
        total = part[x, :, :, at].astype(F32)
        for d in range(1, n_x):
            total = total + xbuf[d - 1, :, :, at].astype(F32)
        total = total.reshape(SLOTS, n_yh, 8, cc).astype(BF16)
        for yi in range(n_yh):
            ysend[yi, :, :, at] = total[:, yi]
        for s in range(SLOTS):
            for e in range(n_yh):
                if s < SLOTS - 1 or e:
                    send(ysend.at[yh_at(e), s, :, at], ybuf.at[(s * n_yh + e + n_yh) % y_n, :, at], ys_sem, yr_sem.at[k],
                         ctx_at(s - 3), yh_at(e) * n_x + x)

    place_here = x * n_yh + yh
    def settle(k):
        at = pl.ds(*chunks[k])
        group(ybuf.at[pl.ds(1, y_n - 1), :, at], ys_sem, yr_sem.at[k]).wait_recv()
        total = ysend[yh, SLOTS - 1, :, at].astype(F32)
        total = total + jnp.sum(ybuf[pl.ds(1, y_n - 1), :, at].astype(F32), axis=0)
        gbuf[place_here, :, at] = total.astype(BF16)

    def spread_out(k):
        at = pl.ds(*chunks[k])
        for d in range(n_x):
            for e in range(n_yh):
                if d or e:
                    send(gbuf.at[place_here, :, at], gbuf.at[place_here, :, at], gs_sem, gr_sem.at[k],
                         c, yh_at(e) * n_x + x_at(d))

    quarter = wid // QUAD
    for k in (0, 1):
        settle(k)
        for to in (2 * k, 2 * k + 1):
            piece = gbuf.at[place_here, :, pl.ds(to * quarter, quarter)]
            by = lax.rem(to + QUAD - quad, QUAD)
            spot = tbuf.at[by * n_head + place_here]
            for d in reversed(range(n_x)):
                for e in reversed(range(n_yh)):
                    if d or e:
                        send(piece, spot, ts_sem, tr_sem, z * QUAD + to, yh_at(e) * n_x + x_at(d))

            @pl.when(quad != to)
            def _():
                send(piece, spot, ts_sem, tr_sem, z * QUAD + to, h)

            @pl.when(quad == to)
            def _():
                tbuf[place_here] = gbuf[place_here, :, pl.ds(to * quarter, quarter)]

    spread_out(0)
    spread_out(1)
    for copy in swap:
        copy.wait_recv()
    t_all = tbuf.at[pl.ds(0, QUAD * n_head - 1)]
    group(t_all, ts_sem, tr_sem).wait_recv()
    square = tbuf[...].astype(F32).reshape(QUAD * tok, quarter).astype(BF16)
    turned = dot((iota((quarter, quarter), 0) == iota((quarter, quarter), 1)).astype(F32).astype(BF16), square, NT)
    turned = turned.astype(BF16)
    total = dot(turned[:, :tok], inp[0], NT)
    for d in (1, 2, 3):
        total = total + dot(turned[:, d * tok:(d + 1) * tok], inp[d], NT)
    zsend[...] = total.reshape(n_z, 8, total.shape[1]).astype(BF16)
    for d in sorted(range(1, n_z), key=lambda d: -min(d, n_z - d)):
        send(zsend.at[lax.rem(z + d, n_z)], zbuf.at[d - 1], zs_sem, zr_sem, z_at(d), h)
    settle(2)
    spread_out(2)
    pl.loop(0, rows // step)(query_grads)
    for k in range(3):
        group(gbuf.at[pl.ds(0, n_head - 1), :, pl.ds(*chunks[k])], gs_sem, gr_sem.at[k]).wait_recv()
    whole = gbuf[...].astype(F32).reshape(tok, full).astype(BF16)
    lg_out[...] = dot(whole[:, :wid], perm[...]).astype(BF16)
    take = (iota((n_rope, EXT), 0) == iota((n_rope, EXT), 1)).astype(F32).astype(BF16)
    krx[...] = dot(take, whole[:, wid:], NT).astype(BF16)
    total = zsend[z].astype(F32)
    for k, (c0, cc) in enumerate(chunks):
        at = pl.ds(c0, cc)
        group(xbuf.at[:, :, :, at], xs_sem, xr_sem.at[k]).wait_send()
        group(ybuf.at[pl.ds(1, y_n - 1), :, at], ys_sem, yr_sem.at[k]).wait_send()
        group(gbuf.at[pl.ds(0, n_head - 1), :, at], gs_sem, gr_sem.at[k]).wait_send()
    group(t_all, ts_sem, tr_sem).wait_send()
    for copy in halo + swap:
        copy.wait_send()
    group(zbuf, zs_sem, zr_sem).wait_recv()
    total = total + jnp.sum(zbuf[...].astype(F32), axis=0)
    pg_out[...] = total
    group(zbuf, zs_sem, zr_sem).wait_send()


def flush(*refs):
    sem = refs[-1]
    copies = [pltpu.make_async_copy(refs[i], refs[i + 5], sem.at[i]) for i in range(5)]
    for copy in copies:
        copy.start()
    for copy in copies:
        copy.wait()


def solution(mesh):
    n_ctx, n_head = mesh.shape["ctx"], mesh.shape["head"]
    n_x = 4 if n_head == 16 else 2
    n_yh = n_head // n_x
    n_z = n_ctx // QUAD

    def shards(q_latent, q_rope, latent, key_rope, out_grad, inputs, doc_ids):
        tok, heads, wid = q_latent.shape
        n_rope, dloc = key_rope.shape[1], inputs.shape[1]
        rows, full, keys = tok * heads, wid + EXT, SLOTS * tok
        cfg = (n_ctx, n_z, n_yh, n_x, tok, wid, heads)
        vm = pltpu.VMEM
        dma = pltpu.SemaphoreType.DMA
        y_n = SLOTS * n_yh
        shape = jax.ShapeDtypeStruct
        anywhere, local = pl.BlockSpec(memory_space=pltpu.HBM), pl.BlockSpec(memory_space=pltpu.VMEM)
        shapes = (
                shape((rows, wid), BF16),
                shape((tok, heads * n_rope), BF16),
                shape((tok, wid), BF16),
                shape((n_rope, tok), BF16),
                shape((8, dloc), F32),
            )
        outs = pl.pallas_call(
            functools.partial(kernel, cfg),
            out_shape=shapes,
            in_specs=[pl.BlockSpec(memory_space=pltpu.HBM)] * 7,
            out_specs=(local,) * 5,
            scratch_shapes=[
                vm((rows, full), BF16), vm((rows, wid), BF16), vm((tok, heads * n_rope), BF16),
                vm((keys, full), BF16), vm((n_rope, tok), BF16), vm((QUAD, dloc, tok), BF16),
                vm((1, tok), jnp.int32), vm((wid, wid), BF16),
                vm((keys, rows), F32), vm((keys, rows), F32), vm((keys, 2 * rows), BF16), vm((2 * rows, full), BF16),
                vm((n_x, SLOTS, tok // n_x, full), BF16), vm((n_x - 1, SLOTS, tok // n_x, full), BF16),
                vm((n_yh, SLOTS, 8, full), BF16), vm((y_n, 8, full), BF16),
                vm((n_head, 8, full), BF16), vm((QUAD * n_head, 8, wid // QUAD), BF16),
                vm((n_z, 8, dloc), BF16), vm((n_z - 1, 8, dloc), BF16),
                vm((tok, EXT), BF16), vm((heads * n_rope, EXT), BF16), vm((EXT, heads * n_rope), BF16),
                dma((7,)), dma((3,)), dma((3,)), dma, dma((3,)), dma, dma((3,)), dma, dma((3,)),
                dma, dma, dma((3,)), dma((3,)), dma, dma,
            ],
            compiler_params=pltpu.CompilerParams(collective_id=0, has_side_effects=True, vmem_limit_bytes=48 << 20),
            name="step",
        )(*(
            pltpu.with_memory_space_constraint(a, pltpu.HBM)
            for a in (q_latent.reshape(rows, wid), q_rope, latent, key_rope.T, out_grad.reshape(rows, wid), inputs.T,
                      doc_ids.reshape(n_ctx, 1, tok))
        ))
        outs = pl.pallas_call(
            flush,
            out_shape=shapes,
            in_specs=[local] * 5,
            out_specs=(anywhere,) * 5,
            scratch_shapes=[dma((5,))],
            compiler_params=pltpu.CompilerParams(vmem_limit_bytes=2 << 20),
            name="flush",
        )(*outs)
        return (outs[0].reshape(tok, heads, wid), outs[1], outs[2], outs[3].T, outs[4])

    return jax.shard_map(
        shards,
        mesh=mesh,
        in_specs=(P("ctx", "head", None), P("ctx", "head"), P("ctx", None), P("ctx", None), P("ctx", "head", None),
                  P("ctx", "head"), P()),
        out_specs=(P("ctx", "head", None), P("ctx", "head"), P("ctx", None), P("ctx", None), P("ctx", "head")),
        check_vma=False,
    )
```
